256 devices in a mesh: shard: 64 (over z, y, core), model: 4 (over x).
Axes of the slice: x: 4, y: 4, z: 8, core: 2. Of those that a mesh axis runs over, the one named last changes fastest.
Arguments:
- one_gate: float32 [2048, 8192], P('shard', 'model'), may hold values from -0.375 to 0.375
- other_gate: float32 [2048, 8192], P('shard', 'model'), may hold values from -0.125 to 0.125
- one_up: float32 [2048, 8192], P('shard', 'model'), may hold values from -0.375 to 0.375
- other_up: float32 [2048, 8192], P('shard', 'model'), may hold values from -0.125 to 0.125
- mix_share: float32 [2048], P('shard'), may hold values from 0.2 to 0.8
- norm_train: float32 [2048], P(('shard', 'model')), may hold values from 0.25 to 1.75
- norm_step: float32 [2048], P(('shard', 'model')), may hold values from -0.3 to 0.3
Outputs:
- final_gate: bfloat16 [2048, 8192], P(None, 'model')
- final_up: bfloat16 [2048, 8192], P(None, 'model')
- column_gate: float32 [8192], P('model')
- column_up: float32 [8192], P('model')
- serve_norm: bfloat16 [2048], replicated
The draws below stay inside these ranges and needn't reach their ends.
All inputs are finite; a program needn't handle non-finite values. Where the reference program divides by a largest or mean magnitude, that divisor is 1e-20 or more.
Results may differ from the reference program's by a relative error of at most 0.001.
Values may be sent and summed in bfloat16 or wider, within the bound.
No kernel may reach another device: no remote copies, remote signals or barrier semaphores. Data moves between devices by JAX's collectives and lax.ppermute only.
A program may use at most 128 MiB of HBM per device.

```python
import jax
import jax.numpy as jnp

D_MODEL = 2048
D_INNER = 8192


def spiked(entries, rng, source, target, blocks, factor):
    def block_of(position):
        return (jnp.arange(entries.shape[position]) // (entries.shape[position] // blocks)).reshape((-1,) + (1,) * (entries.ndim - 1 - position))

    first = jax.random.permutation(rng, blocks)[block_of(target)]
    far = (block_of(target) + blocks // 2) % blocks
    return jnp.where((block_of(source) == first) | (block_of(source) == far), factor * entries, entries)


def level_of(rng, extent, shards, smallest, top_value):
    gain = 1.0
    for axis_at, parts in shards:
        draws = jax.random.uniform(jax.random.fold_in(jax.random.fold_in(rng, 6), axis_at), (parts,), jnp.float32, smallest / len(shards), top_value / len(shards))
        gain = gain * jnp.repeat(jnp.exp(draws), extent[axis_at] // parts).reshape((-1,) + (1,) * (len(extent) - 1 - axis_at))
    return gain


def centred(own_key, shape, scale, reach, split=(), held_as=jnp.bfloat16):
    values = scale * jax.random.normal(own_key, shape, jnp.float32)
    if split:
        values = values * level_of(own_key, shape, split, -0.22, 0.18)
    return jnp.clip(values, -reach, reach).astype(held_as)


def bell_draw_with(own_key, shape, width, limit, shards, heavy, kind=jnp.bfloat16):
    values = width * jax.random.normal(own_key, shape, jnp.float32)
    if shards:
        values = values * level_of(own_key, shape, shards, -0.22, 0.18)
    return jnp.clip(spiked(values, jax.random.fold_in(own_key, 3), *heavy), -limit, limit).astype(kind)


def setup_inputs(seed: int = 0) -> dict:
    keys = jax.random.split(jax.random.key(seed), 8)
    one_gate = bell_draw_with(keys[0], (D_MODEL, D_INNER), D_MODEL ** -0.5, 0.375, ((0, 64), (1, 4)), (0, 1, 64, 4.0), jnp.float32)
    other_gate = centred(keys[1], (D_MODEL, D_INNER), D_MODEL ** -0.5, 0.125, ((0, 64), (1, 4)), jnp.float32)
    one_up = bell_draw_with(keys[2], (D_MODEL, D_INNER), D_MODEL ** -0.5, 0.375, ((0, 64), (1, 4)), (0, 1, 64, 4.0), jnp.float32)
    other_up = centred(keys[3], (D_MODEL, D_INNER), D_MODEL ** -0.5, 0.125, ((0, 64), (1, 4)), jnp.float32)
    mix_share = jnp.clip(0.2 + 0.6 * jax.random.uniform(keys[4], (D_MODEL,), jnp.float32) ** level_of(keys[4], (D_MODEL,), ((0, 64),), -0.2, 0.2), 0.2, 0.8)
    norm_train = jnp.clip(1.0 + 0.15 * jax.random.normal(keys[5], (D_MODEL,), jnp.float32), 0.25, 1.75)
    norm_step = jnp.clip(jax.random.uniform(keys[6], (D_MODEL,), jnp.float32, -0.3, 0.3) * level_of(keys[6], (D_MODEL,), ((0, 256),), -0.4, 0.0), -0.3, 0.3)
    return {"one_gate": one_gate, "other_gate": other_gate, "one_up": one_up, "other_up": other_up, "mix_share": mix_share, "norm_train": norm_train, "norm_step": norm_step}


def reference(one_gate, other_gate, one_up, other_up, mix_share, norm_train, norm_step):
    result_gate = mix_share[:, None] * one_gate + (1.0 - mix_share[:, None]) * other_gate
    result_up = mix_share[:, None] * one_up + (1.0 - mix_share[:, None]) * other_up
    column_gate = jnp.max(jnp.abs(result_gate), axis=0)
    final_gate = (result_gate / column_gate).astype(jnp.bfloat16)
    column_up = jnp.max(jnp.abs(result_up), axis=0)
    final_up = (result_up / column_up).astype(jnp.bfloat16)
    serve_norm = (norm_train + norm_step).astype(jnp.bfloat16)
    return final_gate, final_up, column_gate, column_up, serve_norm
```

```python
import jax
import jax.numpy as jnp
from jax import lax
from jax.sharding import Mesh
from jax.sharding import PartitionSpec as P


SHARD = ("z", "y", "core")
ALL = ("z", "y", "core", "model")
Z, Y, C = 8, 4, 2


def pairs(target):
    at = lambda z, y, c: ((z % Z) * Y + y % Y) * C + c
    return [
        (at(z, y, c), at(*target(z, y, c)))
        for z in range(Z)
        for y in range(Y)
        for c in range(C)
    ]


def way(c):
    return 1 - 2 * c


def along_z(v, k=1):
    return lax.ppermute(v, SHARD, pairs(lambda z, y, c: (z + k * way(c), y, c)))


def along_y(v, k=1):
    return lax.ppermute(v, SHARD, pairs(lambda z, y, c: (z, y + k * way(c), c)))


def swap(v):
    return lax.ppermute(v, "core", [(0, 1), (1, 0)])


def local(one_gate, other_gate, one_up, other_up, mix_share, norm_train, norm_step):
    z, y, c = (lax.axis_index(a) for a in SHARD)
    x = lax.axis_index("model")
    first = c == 0
    s = 2 * c - 1

    share = mix_share[:, None]
    gate = share * one_gate + (1.0 - share) * other_gate
    up = share * one_up + (1.0 - share) * other_up
    mine = jnp.stack([gate, up])
    theirs = swap(mine)

    low = -jnp.inf
    peak = jnp.maximum(jnp.abs(mine).max(1), jnp.abs(theirs).max(1))
    norm = jnp.full((2048,), low, jnp.float32)
    norm = lax.dynamic_update_slice(norm, norm_train + norm_step, ((((z * Y + y) * C + c) * 4 + x) * 8,))
    peak = jnp.concatenate([peak, jnp.maximum(norm, swap(norm))[None]])

    def halved(m):
        return jnp.stack([jnp.where(first, m[0], m[1]), m[2]])

    def widened(h):
        return jnp.stack([jnp.where(first, h[0], low), jnp.where(first, low, h[0]), h[1]])

    one, two = along_y(peak), along_y(halved(peak), 2)
    peak = jnp.maximum(jnp.maximum(peak, one), widened(two))
    peak = jnp.maximum(peak, swap(peak))
    near = [along_z(peak, k) for k in (1, 2, 3)]
    far = along_z(halved(peak), 4)
    for v in near:
        peak = jnp.maximum(peak, v)
    peak = jnp.maximum(peak, widened(far))
    peak = jnp.maximum(peak, swap(peak))
    column_gate, column_up = peak[0], peak[1]

    norm = peak[2]
    for k in (1, 2, 3):
        norm = jnp.maximum(norm, lax.ppermute(peak[2], "model", [(i, (i + k) % 4) for i in range(4)]))
    serve_norm = norm.astype(jnp.bfloat16)

    narrow = (mine / peak[:2, None]).astype(jnp.bfloat16)
    other = (theirs / peak[:2, None]).astype(jnp.bfloat16)
    own = jnp.where(
        first,
        jnp.concatenate([narrow, other], axis=1),
        jnp.concatenate([other, narrow], axis=1),
    )

    out = [jnp.zeros((Z * Y, 64, 2048), jnp.bfloat16) for _ in range(2)]

    def place(which, block, dz, dy):
        row = ((z + dz + Z) % Z) * Y + (y + dy + Y) % Y
        out[which] = lax.dynamic_update_slice(out[which], block.reshape(1, 64, 2048), (row, 0, 0))

    def place_both(v, dz, dy):
        place(0, v[0], dz, dy)
        place(1, v[1], dz, dy)

    place_both(own, 0, 0)
    za = along_z(own)
    y1 = along_y(own)
    y2 = along_y(jnp.where(first, y1[0], y1[1]))
    y1x = swap(y1)
    y2x = swap(y2)
    place_both(y1, 0, s)
    place_both(y1x, 0, -s)
    g2, u2 = jnp.where(first, y2, y2x), jnp.where(first, y2x, y2)
    place(0, g2, 0, 2)
    place(1, u2, 0, 2)
    zb = along_z(jnp.stack([y1[0], y1x[0], g2]))
    for k in (1, 2, 3):
        zax = swap(za)
        place_both(za, k * s, 0)
        place_both(zax, -k * s, 0)
        v = jnp.stack([za[1], zax[1]])
        nxt = za
        za = along_z(nxt) if k < 3 else along_z(jnp.where(first, nxt[0], nxt[1]))
        v1 = along_y(v)
        v2 = along_y(v1[0])
        v1x, v2x = swap(v1), swap(v2)
        place(1, v1[0], k * s, s)
        place(1, v1[1], -k * s, s)
        place(1, v1x[0], -k * s, -s)
        place(1, v1x[1], k * s, -s)
        place(1, v2, k * s, 2)
        place(1, v2x, -k * s, 2)
        zbx = swap(zb)
        for d, w in ((1, zb), (-1, zbx)):
            place(0, w[0], d * k * s, d * s)
            place(0, w[1], d * k * s, -d * s)
            place(0, w[2], d * k * s, 2)
        if k < 3:
            zb = along_z(zb)
        else:
            zb = along_z(jnp.concatenate([zb[0], jnp.where(first, zb[2][:32], zb[2][32:])]))
    zax = swap(za)
    g4, u4 = jnp.where(first, za, zax), jnp.where(first, zax, za)
    place(0, g4, 4, 0)
    place(1, u4, 4, 0)
    v1 = along_y(u4)
    v2 = along_y(jnp.where(first, v1[:32], v1[32:]))
    v1x, v2x = swap(v1), swap(v2)
    place(1, v1, 4, s)
    place(1, v1x, 4, -s)
    place(1, jnp.where(first, jnp.concatenate([v2, v2x]), jnp.concatenate([v2x, v2])), 4, 2)
    zbx = swap(zb)
    place(0, zb[:64], 4, s)
    place(0, zbx[:64], 4, -s)
    place(0, jnp.where(first, jnp.concatenate([zb[64:], zbx[64:]]), jnp.concatenate([zbx[64:], zb[64:]])), 4, 2)
    final_gate, final_up = (o.reshape(2048, 2048) for o in out)
    return final_gate, final_up, column_gate, column_up, serve_norm


def solution(mesh):
    torus = Mesh(mesh.devices.reshape(Z, Y, C, mesh.shape["model"]), ALL)
    return jax.shard_map(
        local,
        mesh=torus,
        in_specs=(P(SHARD, "model"),) * 4 + (P(SHARD), P(ALL), P(ALL)),
        out_specs=(P(None, "model"), P(None, "model"), P("model"), P("model"), P()),
        check_vma=False,
    )
```

```python
import jax
import jax.numpy as jnp
from jax import lax
from jax.experimental import pallas as pl
from jax.experimental.pallas import tpu as pltpu
from jax.sharding import Mesh
from jax.sharding import PartitionSpec as P


SHARD = ("z", "y", "core")
ALL = ("z", "y", "core", "model")
Z, Y, C, X = 8, 4, 2, 4
ROWS = 64
W = 2048
A = 1536


def pairs(target):
    at = lambda z, y, c: ((z % Z) * Y + y % Y) * C + c
    return [
        (at(z, y, c), at(*target(z, y, c)))
        for z in range(Z)
        for y in range(Y)
        for c in range(C)
    ]


def way(c):
    return 1 - 2 * c


def along_z(v, k=1):
    return lax.ppermute(v, SHARD, pairs(lambda z, y, c: (z + k * way(c), y, c)))


def along_y(v, k=1):
    return lax.ppermute(v, SHARD, pairs(lambda z, y, c: (z, y + k * way(c), c)))


def swap(v):
    return lax.ppermute(v, "core", [(0, 1), (1, 0)])


def along_model(v, bit):
    return lax.ppermute(v, "model", [(i, i ^ bit) for i in range(X)])


def at(array, dz, dy, row=0, rows=ROWS, col=0, cols=None, base=0, half=0):
    return (array, dz, dy, row, rows, col, cols or array.shape[1], base, half)


def place(outs, blocks):
    arrays, copies = [], []
    for array, dz, dy, row, rows, col, cols, base, half in blocks:
        which = next((i for i, a in enumerate(arrays) if a is array), None)
        if which is None:
            which = len(arrays)
            arrays.append(array)
        while cols:
            out, start = divmod(base, W)
            width = min(cols, W - start)
            copies.append((which, row, rows, col, width, out, start, dz, dy, half))
            col, base, cols = col + width, base + width, cols - width
    n = len(arrays)

    def kernel(*refs):
        ins, (gate, up), sems = refs[:n], refs[-3:-1], refs[-1]
        z, y, c = (lax.axis_index(a) for a in SHARD)
        side = 2 * c - 1

        def moved(here, step, size):
            step = step[1] * side if isinstance(step, tuple) else step
            return lax.rem(here + step + size, size)

        started = []
        for i, (which, row, rows, col, width, out, start, dz, dy, half) in enumerate(copies):
            to = (moved(z, dz, Z) * Y + moved(y, dy, Y)) * ROWS
            if half:
                to = to + (c if half > 0 else 1 - c) * rows
            to = pl.multiple_of(to, 32)
            copy = pltpu.make_async_copy(
                ins[which].at[row : row + rows, col : col + width],
                (gate, up)[out].at[pl.ds(to, rows), start : start + width],
                sems.at[i],
            )
            copy.start()
            started.append(copy)
        for copy in started:
            copy.wait()

    either, hbm = (pl.BlockSpec(memory_space=m) for m in (pl.ANY, pltpu.HBM))
    shape = jax.ShapeDtypeStruct((Z * Y * ROWS, W), jnp.bfloat16)
    return pl.pallas_call(
        kernel,
        out_shape=(shape, shape),
        in_specs=[either] * n + [hbm] * len(outs),
        out_specs=(hbm, hbm),
        scratch_shapes=[pltpu.SemaphoreType.DMA((len(copies),))],
        input_output_aliases={n + i: i for i in range(len(outs))},
        compiler_params=pltpu.CompilerParams(vmem_limit_bytes=1 << 20),
    )(*arrays, *outs)


def local(one_gate, other_gate, one_up, other_up, mix_share, norm_train, norm_step):
    z, y, c = (lax.axis_index(a) for a in SHARD)
    x = lax.axis_index("model")
    first = c == 0
    low = -jnp.inf
    near, far = ("s", 1), ("s", -1)

    share = mix_share[:, None]
    mine = jnp.concatenate(
        [share * one_gate + (1.0 - share) * other_gate, share * one_up + (1.0 - share) * other_up],
        axis=1,
    )
    theirs = swap(mine)
    own = jnp.where(first, jnp.concatenate([mine, theirs]), jnp.concatenate([theirs, mine]))

    gain = lax.dynamic_update_slice(
        jnp.full((W,), low, jnp.float32), norm_train + norm_step, ((((z * Y + y) * C + c) * X + x) * 8,)
    )
    gain = jnp.maximum(gain, swap(gain))
    peak = jnp.concatenate([jnp.abs(own).max(0), gain])

    def halved(m):
        return jnp.concatenate([jnp.where(first, m[:W], m[W : 2 * W]), m[2 * W :]])

    def widened(h):
        return jnp.concatenate([jnp.where(first, h[:W], low), jnp.where(first, low, h[:W]), h[W:]])

    two, one = along_y(halved(peak), 2), along_y(peak)
    y1r = along_y(own)
    zBr = along_z(own[:, A:])
    peak = jnp.maximum(jnp.maximum(peak, one), widened(two))
    peak = jnp.maximum(peak, swap(peak))
    four = along_z(halved(peak), 4)
    sent = peak
    for k in (3, 2, 1):
        peak = jnp.maximum(peak, along_z(sent, k))
    peak = jnp.maximum(peak, widened(four))
    zAr = along_z(own[:, :A])
    zBxr = swap(zBr)
    y1xr = swap(y1r)
    y2r = along_y(jnp.where(first, y1r[:, :W], y1r[:, W:]))
    zAxr = swap(zAr)
    peak = jnp.maximum(peak, swap(peak))
    y2xr = swap(y2r)

    column = peak[None, : 2 * W]

    def narrow(v, base=0):
        return (v / column[:, base : base + v.shape[1]]).astype(jnp.bfloat16)

    def merged(v, w):
        return jnp.where(first, jnp.concatenate([v, w], axis=1), jnp.concatenate([w, v], axis=1))

    zB, zBx, zA, zAx = narrow(zBr, A), narrow(zBxr, A), narrow(zAr), narrow(zAxr)
    yr1 = along_y(jnp.concatenate([zB, zBx]))
    za2 = along_z(jnp.concatenate([zA, zB], axis=1))
    f0, f1, f1x, f2 = narrow(own), narrow(y1r), narrow(y1xr), narrow(merged(y2r, y2xr))
    zb1 = along_z(jnp.concatenate([f1[:, :A], f1x[:, :A], f2[:, :A]]))
    outs = place(
        (),
        [at(f0, 0, 0), at(f1, 0, near), at(f1x, 0, far), at(f2, 0, 2)]
        + [at(zA, near, 0), at(zAx, far, 0), at(zB, near, 0, base=A), at(zBx, far, 0, base=A)],
    )

    za3 = along_z(za2)
    za2x = swap(za2)
    yh1 = along_y(yr1[:ROWS])
    yr2 = along_y(jnp.concatenate([za2[:, A:], za2x[:, A:]]))
    zb2 = along_z(zb1)
    za4 = along_z(jnp.where(first, za3[:, :W], za3[:, W:]))
    za3x = swap(za3)
    yh2 = along_y(yr2[:ROWS])
    yr3 = along_y(jnp.concatenate([za3[:, A:], za3x[:, A:]]))
    y12 = jnp.concatenate([yr1, yh1, yr2, yh2])
    y12x = swap(y12)
    zb3 = along_z(zb2)
    z12 = jnp.concatenate([zb1, zb2])
    z12x = swap(z12)

    def from_z(v, k, end, row=0):
        d = ("s", k * end)
        return [
            at(v, d, ("s", end), row),
            at(v, d, ("s", -end), row + ROWS),
            at(v, d, 2, row + 2 * ROWS),
        ]

    def from_y(v, k, end, row=0):
        return [
            at(v, ("s", k * end), ("s", end), row, base=A),
            at(v, ("s", -k * end), ("s", end), row + ROWS, base=A),
        ]

    def from_y_half(v, k, end, row=0):
        return [at(v, ("s", k * end), 2, row, base=A)]

    outs = place(
        outs,
        [at(za2, ("s", 2), 0), at(za2x, ("s", -2), 0), at(za3, ("s", 3), 0), at(za3x, ("s", -3), 0)]
        + from_y(yr1, 1, 1) + from_y_half(yh1, 1, 1) + from_y(yr2, 2, 1) + from_y_half(yh2, 2, 1)
        + from_y(y12x, 1, -1) + from_y_half(y12x, 1, -1, 2 * ROWS)
        + from_y(y12x, 2, -1, 3 * ROWS) + from_y_half(y12x, 2, -1, 5 * ROWS),
    )
    za4x = swap(za4)
    f4 = merged(za4, za4x)
    yh3 = along_y(yr3[:ROWS])
    yr4 = along_y(f4[:, A:])
    half = ROWS // 2
    zb4 = along_z(
        jnp.concatenate([zb3[:ROWS], jnp.where(first, zb3[2 * ROWS : -half], zb3[-half:])])
    )
    outs = place(
        outs,
        [at(f4, 4, 0)] + from_z(zb1, 1, 1) + from_z(zb2, 2, 1)
        + from_z(z12x, 1, -1) + from_z(z12x, 2, -1, 3 * ROWS),
    )
    y34 = jnp.concatenate([yr3, yh3, yr4])
    y34x = swap(y34)
    zb3x = swap(zb3)
    yh4 = along_y(jnp.where(first, yr4[:half], yr4[half:]))
    gain = peak[2 * W :]
    gain = jnp.maximum(gain, along_model(gain, 1))
    outs = place(
        outs,
        from_y(yr3, 3, 1) + from_y_half(yh3, 3, 1) + [at(yr4, 4, near, base=A)]
        + from_y(y34x, 3, -1) + from_y_half(y34x, 3, -1, 2 * ROWS) + [at(y34x, 4, far, 3 * ROWS, base=A)]
        + from_z(zb3, 3, 1) + from_z(zb3x, 3, -1),
    )
    zb4x = swap(zb4)
    yh4x = swap(yh4)
    gain = jnp.maximum(gain, along_model(gain, 2))
    final_gate, final_up = place(
        outs,
        [at(zb4, 4, near), at(zb4, 4, 2, ROWS, half, half=1)]
        + [at(zb4x, 4, far), at(zb4x, 4, 2, ROWS, half, half=-1)]
        + [at(yh4, 4, 2, 0, half, base=A, half=1), at(yh4x, 4, 2, 0, half, base=A, half=-1)],
    )
    return final_gate, final_up, peak[:W], peak[W : 2 * W], gain.astype(jnp.bfloat16)


def solution(mesh):
    torus = Mesh(mesh.devices.reshape(Z, Y, C, X), ALL)
    return jax.shard_map(
        local,
        mesh=torus,
        in_specs=(P(SHARD, "model"),) * 4 + (P(SHARD), P(ALL), P(ALL)),
        out_specs=(P(None, "model"), P(None, "model"), P("model"), P("model"), P()),
        check_vma=False,
    )
```
